32 devices in a mesh: lat: 4 (over y, x), lon: 4 (over z), lev: 2 (over core).
Axes of the slice: x: 2, y: 2, z: 4, core: 2. Of those that a mesh axis runs over, the one named last changes fastest.
Arguments:
- field_values: float32 [16, 256, 192, 128], P('lat', 'lon', 'lev'), may hold values from 0.2 to 1.8
- crowding: float32 [16, 256, 192, 128], P('lat', 'lon', 'lev'), may hold values from 0.5 to 2
Outputs:
- field_values_end: float32 [16, 256, 192, 128], P('lat', 'lon', 'lev')
The draws below stay inside these ranges and needn't reach their ends.
All inputs are finite; a program needn't handle non-finite values.
Results may differ from the reference program's by a relative error of at most 0.00002.
Values sent between devices are 32-bit elements; how exact they have to be, the bound alone decides.
No kernel may reach another device: no remote copies, remote signals or barrier semaphores. Data moves between devices by JAX's collectives and lax.ppermute only.
A program may use at most 384 MiB of HBM per device.

```python
import jax
import jax.numpy as jnp
from jax import lax

GRID_J = 16
GRID_I = 256
GRID_K = 192
LEVELS = 128
STEPS = 3


def level_of(stream_key, shape, pieces, least, top_value):
    def one(axis_at, shards_of):
        heights = jax.random.uniform(jax.random.fold_in(jax.random.fold_in(stream_key, 6), axis_at), (shards_of,), jnp.float32, least / len(pieces), top_value / len(pieces))
        return jnp.repeat(jnp.exp(heights), shape[axis_at] // shards_of).reshape((-1,) + (1,) * (len(shape) - axis_at - 1))

    level = one(*pieces[0])
    for cut in pieces[1:]:
        level = level * one(*cut)
    return level


def setup_inputs(seed: int = 0) -> dict:
    arg_keys = jax.random.split(jax.random.key(seed), 3)
    field_values = jnp.clip(0.2 + 1.5999999 * jax.random.uniform(arg_keys[0], (GRID_J, GRID_I, GRID_K, LEVELS), jnp.float32) ** level_of(arg_keys[0], (GRID_J, GRID_I, GRID_K, LEVELS), ((0, 4), (1, 4), (2, 2)), -0.2, 0.2), 0.2, 1.8)
    crowding = jnp.clip(0.5 + 1.5 * jax.random.uniform(arg_keys[1], (GRID_J, GRID_I, GRID_K, LEVELS), jnp.float32) ** level_of(arg_keys[1], (GRID_J, GRID_I, GRID_K, LEVELS), ((0, 4), (1, 4), (2, 2)), -0.2, 0.2), 0.5, 2.0)
    return {"field_values": field_values, "crowding": crowding}


def without_rim(values, dims):
    for dim in dims:
        values = lax.slice_in_dim(values, 1, values.shape[dim] - 1, axis=dim)
    return values


def shifted_cells(values, dim, start, dims):
    others = [other for other in dims if other != dim]
    values = without_rim(values, others)
    return lax.slice_in_dim(values, start, start + values.shape[dim] - 2, axis=dim)


def march_step(padded, crowding):
    middle = without_rim(padded, (0, 1, 2))
    lower = [shifted_cells(padded, dim, 0, (0, 1, 2)) for dim in (0, 1, 2)]
    upper = [shifted_cells(padded, dim, 2, (0, 1, 2)) for dim in (0, 1, 2)]
    spread = lower[0] + upper[0] + lower[1] + upper[1] + lower[2] + upper[2] - 6.0 * middle
    return middle + 0.1 * spread + 0.2 * middle * (1.0 - middle * crowding)


def reference(field_values, crowding):
    for step in range(STEPS):
        field_values = march_step(jnp.pad(field_values, ((1, 1), (1, 1), (1, 1), (0, 0)), mode="wrap"), crowding)
    return field_values
```

```python
import functools

import jax
import jax.numpy as jnp
from jax import lax
from jax.experimental import pallas as pl
from jax.experimental.pallas import tpu as pltpu
from jax.sharding import PartitionSpec as P

STEPS = 3


def ring(axis):
    count = lax.axis_size(axis)
    forward = [(i, (i + 1) % count) for i in range(count)]
    return forward, [(target, source) for source, target in forward]


def send_up(values, axis):
    return lax.ppermute(values, axis, ring(axis)[0])


def send_down(values, axis):
    return lax.ppermute(values, axis, ring(axis)[1])


def swap_k(edges):
    if lax.axis_size("lev") == 2:
        return lax.ppermute(edges, "lev", ring("lev")[0])
    return jnp.stack([send_down(edges[0], "lev"), send_up(edges[1], "lev")])


def row_kernel(*refs, chunk, first, total, with_edges):
    below, mid, above, before, after, crowd, i_low, i_high, k_in = refs[:9]
    outs = refs[len(refs) - (2 if with_edges else 1):]
    out = outs[0]
    at = pl.program_id(0) + first
    cells = mid.shape[2]
    place = lax.broadcasted_iota(jnp.int32, mid.shape[2:], 0)
    k_above = k_in[0]
    k_below = k_in[1]
    starts, ends = [], []
    for i in range(chunk):
        m = mid[0, i]
        if i > 0:
            low = mid[0, i - 1]
        else:
            low = jnp.where(at == 0, i_low[0, 0], before[0, 0])
        if i < chunk - 1:
            high = mid[0, i + 1]
        else:
            high = jnp.where(at == total - 1, i_high[0, 0], after[0, 0])
        k_low = jnp.where(place == 0, k_below[i:i + 1], pltpu.roll(m, 1, 0))
        k_high = jnp.where(place == cells - 1, k_above[i:i + 1], pltpu.roll(m, cells - 1, 0))
        around = (below[0, i] + above[0, i]) + (low + high) + (k_low + k_high)
        new = m * (0.6 - 0.2 * (m * crowd[0, i])) + 0.1 * around
        out[0, i] = new
        if with_edges:
            outs[1][0, i:i + 1, :] = new[0:1]
            outs[1][1, i:i + 1, :] = new[cells - 1:cells]


def row_step(below, mid, above, crowd, i_low, i_high, k_in, *, span=None, out=None,
             out_rows=1, out_row=0, with_edges=True, order=()):
    cells_i, cells_k, levels = mid[0].shape[1:]
    chunk = 8 if cells_i % 8 == 0 else cells_i
    total = cells_i // chunk
    start, stop = span or (0, cells_i)
    first, steps = start // chunk, (stop - start) // chunk

    def row(pair):
        array, j = pair
        shift = first if array.shape[1] == cells_i else 0
        return pl.BlockSpec((1, chunk, cells_k, levels), lambda g: (j, g + shift, 0, 0))

    def one(pair, index):
        array, j = pair
        return pl.BlockSpec((1, 1, cells_k, levels), lambda g: (j, index(g), 0, 0))

    edge = pl.BlockSpec((2, chunk, levels), lambda g: (0, g + first, 0))
    whole = pl.BlockSpec(memory_space=pl.ANY)
    operands = [below[0], mid[0], above[0], mid[0], mid[0], crowd[0], i_low[0], i_high[0], k_in]
    specs = [
        row(below), row(mid), row(above),
        one(mid, lambda g: jnp.maximum((g + first) * chunk - 1, 0)),
        one(mid, lambda g: jnp.minimum((g + first + 1) * chunk, cells_i - 1)),
        row(crowd), one(i_low, lambda g: 0), one(i_high, lambda g: 0), edge,
    ]
    aliases = {}
    out_shape = [jax.ShapeDtypeStruct((out_rows, cells_i, cells_k, levels), mid[0].dtype)]
    out_specs = [pl.BlockSpec((1, chunk, cells_k, levels), lambda g: (out_row, g + first, 0, 0))]
    if with_edges:
        out_shape.append(jax.ShapeDtypeStruct((2, cells_i, levels), mid[0].dtype))
        out_specs.append(edge)
    if out is not None:
        for n, array in enumerate(out):
            aliases[len(operands)] = n
            operands.append(array)
            specs.append(whole)
    for array in order:
        operands.append(array)
        specs.append(whole)
    return pl.pallas_call(
        functools.partial(row_kernel, chunk=chunk, first=first, total=total, with_edges=with_edges),
        grid=(steps,), in_specs=specs, out_specs=out_specs, out_shape=out_shape,
        input_output_aliases=aliases,
    )(*operands)


def tail_spans(cells):
    chunk = 8 if cells % 8 == 0 else cells
    return [(0, cells)] if chunk == cells else [(0, cells - chunk), (cells - chunk, cells)]


def local(field_values, crowding):
    rows, cells_i = field_values.shape[:2]
    last = rows - 1
    tail = tail_spans(cells_i)

    below = [(send_up(field_values[last:], "lat"), (0, cells_i))]
    above = [(send_down(field_values[:1], "lat"), (0, cells_i))]
    i_low0 = send_up(field_values[:, cells_i - 1:], "lon")
    i_high0 = send_down(field_values[:, :1], "lon")
    k_edge0 = jnp.stack([field_values[:, :, 0], field_values[:, :, -1]], axis=1)
    k_in0 = [swap_k(k_edge0[j]) for j in range(rows)]

    now = [(field_values, j) for j in range(rows)]
    i_low = [(i_low0, j) for j in range(rows)]
    i_high = [(i_high0, j) for j in range(rows)]
    k_in = k_in0
    token = ()
    out = None
    for step in range(STEPS):
        final = step == STEPS - 1
        new = [None] * rows
        edges = [None] * rows

        def advance(j, low, high, order):
            nonlocal out
            pieces = low if j == 0 else high if j == last else [(None, (0, cells_i))]
            made = None
            for side, span in pieces:
                made = row_step(
                    (side, 0) if j == 0 else now[j - 1], now[j],
                    (side, 0) if j == last else now[j + 1],
                    (crowding, j), i_low[j], i_high[j], k_in[j], span=span,
                    out=(None if out is None else [out]) if final else made,
                    out_rows=rows if final else 1, out_row=j if final else 0,
                    with_edges=not final, order=order)
                if final:
                    out = made[0]
                order = ()
            if final:
                return ()
            new[j] = (made[0], 0)
            edges[j] = made[1]
            return (made[1],)

        low_first = step % 2 == 0
        order_of = [0, last] if low_first else [last, 0]
        inner = list(range(1, last))
        next_below = next_above = None
        for j in inner:
            token = advance(j, below, above, token)
        for n, j in enumerate(order_of):
            token = advance(j, below, above, token)
            if final:
                continue
            spans = tail if step == STEPS - 2 and n == 1 else [(0, cells_i)]
            sent = [(new[j][0][:, a:b], (a, b)) for a, b in spans]
            if j == 0:
                next_above = [(send_down(values, "lat"), span) for values, span in sent]
            else:
                next_below = [(send_up(values, "lat"), span) for values, span in sent]
        if final:
            break
        i_low = [(send_up(new[j][0][:, cells_i - 1:], "lon"), 0) for j in range(rows)]
        i_high = [(send_down(new[j][0][:, :1], "lon"), 0) for j in range(rows)]
        k_in = [swap_k(edges[j]) for j in range(rows)]
        now, below, above = new, next_below, next_above
    return out


def solution(mesh):
    placed = (P("lat", "lon", "lev", None), P("lat", "lon", "lev", None))
    return jax.shard_map(
        local, mesh=mesh, in_specs=placed, out_specs=P("lat", "lon", "lev", None), check_vma=False
    )
```

```python
import functools

import jax
import jax.numpy as jnp
from jax import lax
from jax.experimental import pallas as pl
from jax.experimental.pallas import tpu as pltpu
from jax.sharding import PartitionSpec as P


STEPS = 3


def ring(axis):
    count = lax.axis_size(axis)
    forward = [(i, (i + 1) % count) for i in range(count)]
    return forward, [(target, source) for source, target in forward]


def send_up(values, axis):
    return lax.ppermute(values, axis, ring(axis)[0])


def send_down(values, axis):
    return lax.ppermute(values, axis, ring(axis)[1])


def swap_k(edges):
    if lax.axis_size("lev") == 2:
        return lax.ppermute(edges, "lev", ring("lev")[0])
    return jnp.stack([send_down(edges[0], "lev"), send_up(edges[1], "lev")])


def row_kernel(*refs, chunk, first, total, with_edges):
    below, mid, above, before, after, crowd, i_low, i_high, k_in = refs[:9]
    outs = refs[len(refs) - (2 if with_edges else 1):]
    out = outs[0]
    at = pl.program_id(0) + first
    cells = mid.shape[2]
    place = lax.broadcasted_iota(jnp.int32, mid.shape[2:], 0)
    k_above = k_in[0]
    k_below = k_in[1]
    for i in range(chunk):
        m = mid[0, i]
        if i > 0:
            low = mid[0, i - 1]
        else:
            low = jnp.where(at == 0, i_low[0, 0], before[0, 0])
        if i < chunk - 1:
            high = mid[0, i + 1]
        else:
            high = jnp.where(at == total - 1, i_high[0, 0], after[0, 0])
        k_low = jnp.where(place == 0, k_below[i:i + 1], pltpu.roll(m, 1, 0))
        k_high = jnp.where(place == cells - 1, k_above[i:i + 1], pltpu.roll(m, cells - 1, 0))
        around = (below[0, i] + above[0, i]) + (low + high) + (k_low + k_high)
        new = m * (0.6 - 0.2 * (m * crowd[0, i])) + 0.1 * around
        out[0, i] = new
        if with_edges:
            outs[1][0, i:i + 1, :] = new[0:1]
            outs[1][1, i:i + 1, :] = new[cells - 1:cells]


def row_step(below, mid, above, crowd, i_low, i_high, k_in, *, span=None, out=None,
             out_rows=1, out_row=0, with_edges=True, order=()):
    cells_i, cells_k, levels = mid[0].shape[1:]
    chunk = 8 if cells_i % 8 == 0 else cells_i
    total = cells_i // chunk
    start, stop = span or (0, cells_i)
    first, steps = start // chunk, (stop - start) // chunk

    def row(pair):
        array, j = pair
        shift = first if array.shape[1] == cells_i else 0
        return pl.BlockSpec((1, chunk, cells_k, levels), lambda g: (j, g + shift, 0, 0))

    def one(pair, index):
        _, j = pair
        return pl.BlockSpec((1, 1, cells_k, levels), lambda g: (j, index(g), 0, 0))

    edge = pl.BlockSpec((2, chunk, levels), lambda g: (0, g + first, 0))
    whole = pl.BlockSpec(memory_space=pl.ANY)
    operands = [below[0], mid[0], above[0], mid[0], mid[0], crowd[0], i_low[0], i_high[0], k_in]
    specs = [
        row(below), row(mid), row(above),
        one(mid, lambda g: jnp.maximum((g + first) * chunk - 1, 0)),
        one(mid, lambda g: jnp.minimum((g + first + 1) * chunk, cells_i - 1)),
        row(crowd), one(i_low, lambda g: 0), one(i_high, lambda g: 0), edge,
    ]
    aliases = {}
    out_shape = [jax.ShapeDtypeStruct((out_rows, cells_i, cells_k, levels), mid[0].dtype)]
    out_specs = [pl.BlockSpec((1, chunk, cells_k, levels), lambda g: (out_row, g + first, 0, 0))]
    if with_edges:
        out_shape.append(jax.ShapeDtypeStruct((2, cells_i, levels), mid[0].dtype))
        out_specs.append(edge)
    if out is not None:
        for n, array in enumerate(out):
            aliases[len(operands)] = n
            operands.append(array)
            specs.append(whole)
    for array in order:
        operands.append(array)
        specs.append(whole)
    return pl.pallas_call(
        functools.partial(row_kernel, chunk=chunk, first=first, total=total, with_edges=with_edges),
        grid=(steps,), in_specs=specs, out_specs=out_specs, out_shape=out_shape,
        input_output_aliases=aliases,
    )(*operands)


def tail_spans(cells):
    chunk = 8 if cells % 8 == 0 else cells
    return [(0, cells)] if chunk == cells else [(0, cells - chunk), (cells - chunk, cells)]


def head_spans(cells):
    chunk = 8 if cells % 8 == 0 else cells
    return [(0, cells)] if chunk == cells else [(0, chunk), (chunk, cells)]


def local(field_values, crowding):
    rows, cells_i = field_values.shape[:2]
    last = rows - 1
    tail = tail_spans(cells_i)

    below = []
    for a, b in head_spans(cells_i):
        below.append((send_up(field_values[last:, a:b], "lat"), (a, b)))
    above = [(send_down(field_values[:1], "lat"), (0, cells_i))]
    i_low0 = send_up(field_values[:, cells_i - 1:], "lon")
    i_high0 = send_down(field_values[:, :1], "lon")
    k_edge0 = jnp.stack([field_values[:, :, 0], field_values[:, :, -1]], axis=1)
    k_in0 = [swap_k(k_edge0[j]) for j in range(rows)]

    now = [(field_values, j) for j in range(rows)]
    i_low = [(i_low0, j) for j in range(rows)]
    i_high = [(i_high0, j) for j in range(rows)]
    k_in = k_in0
    token = ()
    out = None
    for step in range(STEPS):
        final = step == STEPS - 1
        new = [None] * rows
        edges = [None] * rows

        def advance(j, low, high, order):
            nonlocal out
            pieces = low if j == 0 else high if j == last else [(None, (0, cells_i))]
            made = None
            for side, span in pieces:
                made = row_step(
                    (side, 0) if j == 0 else now[j - 1], now[j],
                    (side, 0) if j == last else now[j + 1],
                    (crowding, j), i_low[j], i_high[j], k_in[j], span=span,
                    out=(None if out is None else [out]) if final else made,
                    out_rows=rows if final else 1, out_row=j if final else 0,
                    with_edges=not final, order=order)
                if final:
                    out = made[0]
                order = ()
            if final:
                return ()
            new[j] = (made[0], 0)
            edges[j] = made[1]
            return (made[1],)

        low_first = step % 2 == 0
        order_of = [0, last] if low_first else [last, 0]
        inner = list(range(1, last))
        next_below = next_above = None
        for j in inner:
            token = advance(j, below, above, token)
        for n, j in enumerate(order_of):
            token = advance(j, below, above, token)
            if final:
                continue
            spans = tail if step == STEPS - 2 and n == 1 else [(0, cells_i)]
            sent = [(new[j][0][:, a:b], (a, b)) for a, b in spans]
            if j == 0:
                next_above = [(send_down(values, "lat"), span) for values, span in sent]
            else:
                next_below = [(send_up(values, "lat"), span) for values, span in sent]
        if final:
            break
        i_low = [(send_up(new[j][0][:, cells_i - 1:], "lon"), 0) for j in range(rows)]
        i_high = [(send_down(new[j][0][:, :1], "lon"), 0) for j in range(rows)]
        k_in = [swap_k(edges[j]) for j in range(rows)]
        now, below, above = new, next_below, next_above
    return out


def solution(mesh):
    placed = (P("lat", "lon", "lev", None), P("lat", "lon", "lev", None))
    return jax.shard_map(
        local, mesh=mesh, in_specs=placed, out_specs=P("lat", "lon", "lev", None), check_vma=False
    )
```
